32 devices in a mesh: pitch: 4 (over x, core), span: 8 (over z, y).
Axes of the slice: x: 2, y: 2, z: 4, core: 2. Of those that a mesh axis runs over, the one named last changes fastest.
Arguments:
- residual: float32 [5, 4, 64, 1024], P(None, None, 'span', 'pitch'), may hold values from -0.6 to 0.6
- inverse_diagonal: float32 [5, 5, 4, 64, 1024], P(None, None, None, 'span', 'pitch'), may hold values from -0.1 to 1, as said below
- prior_increment: float32 [5, 4, 64, 1024], P(None, None, 'span', 'pitch'), may hold values from -3 to 3
- coupling: float32 [6, 5, 5], replicated, may hold values from -1 to 1
- characteristic: float32 [2, 2, 512, 5, 5], replicated, may hold values from -6 to 6
- cutoffs: int32 [2], replicated, may hold values from 128 to 512
Outputs:
- update: float32 [5, 4, 64, 1024], P(None, None, 'span', 'pitch')
The draws below stay inside these ranges and needn't reach their ends.
Inputs may be any that keep to these rules, and one draw needn't show every extreme that they name: `inverse_diagonal`: each cell's block is dominated by its diagonal; the sweeps' recurrences are stable.
All inputs are finite; a program needn't handle non-finite values.
Results may differ from the reference program's by a relative error of at most 0.0003.
Values sent between devices are 32-bit elements; how exact they have to be, the bound alone decides.
A program may use at most 64 MiB of HBM per device.

```python
import jax
import jax.numpy as jnp
from jax import lax

VARIABLES = 5
NP = 1024
HARMONICS = 512
AXIAL = 4
SPANWISE_VOLUMES = 64


def draw_inverse_diagonal(key, part):
    first_key, interaction_seed, third_key = jax.random.split(jax.random.fold_in(key, 11), 3)
    shape = (VARIABLES, AXIAL, SPANWISE_VOLUMES, NP)
    spread = jax.random.uniform(first_key, shape, jnp.float32, 0.0, 0.004)
    relaxation_passes = jax.random.randint(interaction_seed, (2,), 0, SPANWISE_VOLUMES)
    spanwise_location = jnp.arange(SPANWISE_VOLUMES, dtype=jnp.int32)
    affected_volumes = jnp.any(spanwise_location[:, None] == relaxation_passes[None, :], axis=1)
    factor = jnp.where(affected_volumes, 0.75, 1.0).astype(jnp.float32)[None, None, :, None]
    diagonal = jnp.exp(-spread) * factor
    full_shape = (VARIABLES, VARIABLES, AXIAL, SPANWISE_VOLUMES, NP)
    offdiag = jnp.clip(0.03 * jax.random.normal(third_key, full_shape, jnp.float32), -0.1, 0.1)
    identity = jnp.eye(VARIABLES, dtype=jnp.float32)[:, :, None, None, None]
    return offdiag * (1.0 - identity) + identity * diagonal[:, None]


def draw_coupling(key, part):
    keys = jax.random.split(jax.random.fold_in(key, 23), 4)
    order = jax.random.permutation(keys[0], VARIABLES)
    slow = order < 3
    rates = jnp.where(slow, 0.998, 0.9).astype(jnp.float32)
    lower_part = jnp.tril(0.05 * jax.random.normal(keys[1], (VARIABLES, VARIABLES), jnp.float32), -1)
    upper_part = jnp.tril(0.05 * jax.random.normal(keys[2], (VARIABLES, VARIABLES), jnp.float32), -1)
    radial_lower = -(jnp.diag(rates) + lower_part)
    radial_upper = jnp.diag(rates) + upper_part
    others = jnp.clip(0.1 * jax.random.normal(keys[3], (4, VARIABLES, VARIABLES), jnp.float32), -0.4, 0.4)
    return jnp.concatenate([radial_lower[None], radial_upper[None], others], axis=0)


def block_scale(rng, shape, pieces, low, high):
    def one(position, parts):
        steps = jax.random.uniform(jax.random.fold_in(jax.random.fold_in(rng, 6), position), (parts,), jnp.float32, low / len(pieces), high / len(pieces))
        return jnp.repeat(jnp.exp(steps), shape[position] // parts).reshape((-1,) + (1,) * (len(shape) - position - 1))

    gain = one(*pieces[0])
    for cut in pieces[1:]:
        gain = gain * one(*cut)
    return gain


def bell_draw(rng, extent, deviation, limit, cuts=(), kind=jnp.bfloat16):
    loudness = block_scale(rng, extent, cuts, -0.22, 0.18) if cuts else 1.0
    values = jax.random.normal(rng, extent, jnp.float32) * deviation * loudness
    return jnp.minimum(jnp.maximum(values, -limit), limit).astype(kind)


def setup_inputs(seed: int = 0) -> dict:
    streams_of = jax.random.split(jax.random.key(seed), 7)
    residual = bell_draw(streams_of[0], (VARIABLES, AXIAL, SPANWISE_VOLUMES, NP), 0.1, 0.6, ((2, 8), (3, 4)), jnp.float32)
    inverse_diagonal = draw_inverse_diagonal(jax.random.fold_in(streams_of[6], 71), 0)
    prior_increment = bell_draw(streams_of[2], (VARIABLES, AXIAL, SPANWISE_VOLUMES, NP), 0.5, 3.0, ((2, 8), (3, 4)), jnp.float32)
    coupling = draw_coupling(jax.random.fold_in(streams_of[6], 71), 0)
    characteristic = bell_draw(streams_of[4], (2, 2, HARMONICS, VARIABLES, VARIABLES), 1.0, 6.0, (), jnp.float32)
    cutoffs = jax.random.randint(streams_of[5], (2,), HARMONICS // 4, HARMONICS + 1).astype(jnp.int32)
    return {"residual": residual, "inverse_diagonal": inverse_diagonal, "prior_increment": prior_increment, "coupling": coupling, "characteristic": characteristic, "cutoffs": cutoffs}


highest = lax.Precision.HIGHEST


def angle_tables(pitch_index, harmonic_index, points):
    product = (pitch_index[:, None] * harmonic_index[None, :]) % points
    angles = product.astype(jnp.float32) * (2.0 * jnp.pi / points)
    return jnp.cos(angles), jnp.sin(angles)


def forward_dft(spanwise_slices, cosine, sine):
    flat = spanwise_slices.reshape(-1, spanwise_slices.shape[-1])
    shape = spanwise_slices.shape[:-1] + (cosine.shape[1],)
    real_part = jnp.dot(flat, cosine, precision=highest).reshape(shape)
    imag_part = -jnp.dot(flat, sine, precision=highest).reshape(shape)
    return real_part, imag_part


def contract(matrix, spectrum):
    return jnp.einsum('pkij,pjrk->pirk', matrix, spectrum, precision=highest)


def apply_harmonics(real_part, imag_part, characteristic, cutoffs, first_harmonic, points):
    char_real = characteristic[:, 0]
    char_imag = characteristic[:, 1]
    result_real_component = contract(char_real, real_part) - contract(char_imag, imag_part)
    out_imag = contract(char_real, imag_part) + contract(char_imag, real_part)
    harmonic = first_harmonic + jnp.arange(real_part.shape[-1], dtype=jnp.int32)
    kept = (harmonic[None, :] < cutoffs[:, None]).astype(jnp.float32)
    weight = jnp.where(harmonic == 0, 1.0, 2.0).astype(jnp.float32) / points
    factor = (kept * weight[None, :])[:, None, None, :]
    return result_real_component * factor, out_imag * factor


def inverse_dft(result_real_component, out_imag, cosine, sine):
    shape = result_real_component.shape[:-1] + (cosine.shape[0],)
    flat_real = result_real_component.reshape(-1, result_real_component.shape[-1])
    flat_imag = out_imag.reshape(-1, out_imag.shape[-1])
    result = jnp.dot(flat_real, cosine.T, precision=highest) - jnp.dot(flat_imag, sine.T, precision=highest)
    return result.reshape(shape)


def mix_field(matrix, field):
    return jnp.einsum('ij,jarp->iarp', matrix, field, precision=highest)


def mix_vector(matrix, vector):
    return jnp.einsum('ij,jap->iap', matrix, vector, precision=highest)


def apply_block(block, vector):
    return jnp.einsum('ijap,jap->iap', block, vector, precision=highest)


def reference(residual, inverse_diagonal, prior_increment, coupling, characteristic, cutoffs):
    spanwise_slices = jnp.stack([residual[:, 0], residual[:, -1]])
    pitch_index = jnp.arange(NP, dtype=jnp.int32)
    harmonic_index = jnp.arange(HARMONICS, dtype=jnp.int32)
    cosine, sine = angle_tables(pitch_index, harmonic_index, NP)
    real_part, imag_part = forward_dft(spanwise_slices, cosine, sine)
    result_real_component, out_imag = apply_harmonics(real_part, imag_part, characteristic, cutoffs, 0, NP)
    correction = inverse_dft(result_real_component, out_imag, cosine, sine)
    corrected = residual.at[:, 0].add(correction[0]).at[:, -1].add(correction[1])
    padded = jnp.concatenate([prior_increment[..., -1:], prior_increment, prior_increment[..., :1]], axis=3)
    axial_pad = jnp.pad(prior_increment, ((0, 0), (1, 1), (0, 0), (0, 0)))
    source = corrected - mix_field(coupling[2], padded[..., :-2]) - mix_field(coupling[3], padded[..., 2:])
    source = source - mix_field(coupling[4], axial_pad[:, :-2]) - mix_field(coupling[5], axial_pad[:, 2:])
    diag_rows = jnp.moveaxis(inverse_diagonal, 3, 0)
    source_rows = jnp.moveaxis(source, 2, 0)
    zeros = jnp.zeros((residual.shape[0], residual.shape[1], residual.shape[3]), jnp.float32)

    def forward_sweep_step(previous, pair):
        block, rhs_row = pair
        current = apply_block(block, rhs_row - mix_vector(coupling[0], previous))
        return current, current

    _, star_rows = lax.scan(forward_sweep_step, zeros, (diag_rows, source_rows))

    def backward_step(following, pair):
        block, star_row = pair
        current = star_row - apply_block(block, mix_vector(coupling[1], following))
        return current, current

    _, final_rows = lax.scan(backward_step, zeros, (diag_rows, star_rows), reverse=True)
    return jnp.moveaxis(final_rows, 0, 2)
```

```python
import jax
import jax.numpy as jnp
import numpy as np
from jax import lax
from jax.experimental import pallas as pl
from jax.experimental.pallas import tpu as pltpu
from jax.sharding import PartitionSpec as P

LANES = 128
SUBLANES = 8
VMEM = pltpu.VMEM
SMEM = pltpu.SMEM
DMA = pltpu.SemaphoreType.DMA
MAPS = 80
EARLY = 88
PAIR = 16
F32 = jnp.float32
BF16 = jnp.bfloat16


def total(terms):
    result = terms[0]
    for term in terms[1:]:
        result = result + term
    return result


def tree(terms):
    while len(terms) > 1:
        terms = [
            terms[i] + terms[i + 1] if i + 1 < len(terms) else terms[i]
            for i in range(0, len(terms), 2)
        ]
    return terms[0]


def times(block, vector, nv):
    return [tree([block[i][j] * vector[j] for j in range(nv)]) for i in range(nv)]


def remote(src, dst, send, recv, device):
    return pltpu.make_async_remote_copy(
        src_ref=src,
        dst_ref=dst,
        send_sem=send,
        recv_sem=recv,
        device_id=device,
        device_id_type=pl.DeviceIdType.MESH,
    )


def split_dot(value, high, low):
    rows = value.shape[0]
    head = value.astype(BF16)
    rest = (value - head.astype(F32)).astype(BF16)
    both = jnp.dot(jnp.concatenate([head, rest]), high, preferred_element_type=F32)
    return both[:rows] + both[rows:] + jnp.dot(head, low, preferred_element_type=F32)


def tables(points, harmonics):
    quarter = points // 4
    p = np.arange(quarter)[:, None]
    blocks = []
    for s in range(4):
        angle = (p * (4 * np.arange(harmonics // 4)[None, :] + s) % points) * (2.0 * np.pi / points)
        blocks.append(np.concatenate([np.cos(angle), np.sin(angle)], axis=1))
    full = np.concatenate(blocks, axis=1).astype(np.float32)
    high = full.astype(BF16)
    low = (full - high.astype(np.float32)).astype(BF16)
    forward = np.stack([high, low])
    return forward, np.ascontiguousarray(forward.transpose(0, 2, 1))


def kernel(
    nv, axial, rows, cw, harmonics,
    cutoffs, coupling, res_in, prior_in, diag_in, char_in, fwd_in, inv_in,
    out,
    res, prior, diag, char, fwd, inv,
    stage, lines, edge, edges, entries, chars,
    low_steps, up_steps, grown, src, base, send_maps, send_pair,
    got_late, got_early, got_pair, solved_early, solved_late, back,
    corr_send, corr_got,
    in_sem, line_send, line_recv, edge_send, edge_recv, corr_ssem, corr_rsem,
    late_send, late_recv, early_send, early_recv, pair_send, pair_recv,
    re_send, re_recv, rl_send, rl_recv,
):
    n = lax.axis_size("pitch")
    m = lax.axis_size("span")
    me = lax.axis_index("pitch")
    mine = lax.axis_index("span")
    core = lax.rem(me, 2)
    chip = me // 2
    cells = axial * cw
    nn = nv * nv
    half = rows // 2
    count = nv * 2 * half
    owners = 2 * cw
    first = m // 2 - owners // 2
    own = mine - first
    is_owner = jnp.logical_and(own >= 0, own < owners)

    def late_row(k):
        return jnp.where(k < cw, k, cells - 2 * cw + k) if not isinstance(k, int) else (
            k if k < cw else cells - 2 * cw + k)

    def early_row(k):
        return cw + k

    copies = [
        pltpu.make_async_copy(a, b, in_sem.at[i])
        for i, (a, b) in enumerate(
            [(res_in, res), (prior_in, prior), (diag_in, diag), (char_in, char),
             (fwd_in, fwd), (inv_in, inv)]
        )
    ]
    for copy in copies:
        copy.start()
    get_res, get_prior, get_diag, get_char, get_fwd, get_inv = copies

    barrier = pltpu.get_barrier_semaphore()

    def greet(axis, to):
        pl.semaphore_signal(
            barrier, inc=1, device_id={axis: to}, device_id_type=pl.DeviceIdType.MESH
        )

    for step in range(1, n):
        greet("pitch", lax.rem(me + step, n))

    @pl.when(is_owner)
    def _():
        for step in range(1, m):
            greet("span", lax.rem(mine + step, m))

    @pl.when(jnp.logical_not(is_owner))
    def _():
        for k in range(owners):
            greet("span", first + k)

    def tile(ref, i, a, c):
        at = ((i * axial + a) * cw + c) * rows
        return ref[at:at + rows, :]

    get_res.wait()
    for h in range(2):
        for c in range(cw):
            for i in range(nv):
                for q in range(2):
                    a = 0 if q == 0 else axial - 1
                    at = ((i * axial + a) * cw + c) * rows + h * half
                    to = c * count + i * 2 * half + q * half
                    stage[h, to:to + half, :] = res[at:at + half, :]

    get_prior.wait()
    lane = lax.broadcasted_iota(jnp.int32, (rows, LANES), 1)
    packed = jnp.zeros((rows, LANES), F32)
    for j in range(nv):
        for a in range(axial):
            at = j * axial + a
            left = jnp.broadcast_to(tile(prior, j, a, 0)[:, 0:1], (rows, LANES))
            right = jnp.broadcast_to(tile(prior, j, a, cw - 1)[:, LANES - 1:], (rows, LANES))
            packed = jnp.where(lane == at, left, packed)
            packed = jnp.where(lane == nv * axial + at, right, packed)
    edge[...] = packed

    @pl.when(is_owner)
    def _():
        pl.semaphore_wait(barrier, n - 1 + m - 1)

    @pl.when(jnp.logical_not(is_owner))
    def _():
        pl.semaphore_wait(barrier, n - 1 + owners)

    gather = []
    for step in [s for s in range(2, n)] + [1]:
        to = jnp.bitwise_xor(me, step)
        gather.append(
            remote(
                stage.at[lax.rem(to, 2)], lines.at[me], line_send.at[step - 1],
                line_recv.at[step - 1], {"pitch": to},
            )
        )
        gather[-1].start()
    after = lax.rem(me + 1, n)
    before = lax.rem(me + n - 1, n)
    edge_copies = [
        remote(edge, edges.at[0], edge_send.at[0], edge_recv.at[0], {"pitch": after}),
        remote(edge, edges.at[1], edge_send.at[1], edge_recv.at[1], {"pitch": before}),
    ]
    for copy in edge_copies:
        copy.start()
    lines[me] = stage[core]

    get_diag.wait()
    zero = jnp.zeros((cells, LANES), F32)
    one = jnp.ones((cells, LANES), F32)
    identity = [one if i == j else zero for j in range(nv) for i in range(nv)]

    def cell_row(ref, at, row):
        return ref[pl.ds(at * cells * rows + row, cells, stride=rows), :]

    def block_at(row):
        return [[cell_row(diag, i * nv + j, row) for j in range(nv)] for i in range(nv)]

    def entry(which, i, j):
        return coupling[(which * nv + i) * nv + j]

    def steps_at(ref, row):
        return [[ref[row, i * nv + j] for j in range(nv)] for i in range(nv)]

    def advance(ref, row, carry):
        step = steps_at(ref, row)
        new = []
        for j in range(nv):
            new += times(step, carry[j * nv:(j + 1) * nv], nv)
        return new

    def prepare(row, carry):
        block = block_at(row)
        for ref, which in ((low_steps, 0), (up_steps, 1)):
            for k in range(nv):
                column = [-entry(which, j, k) for j in range(nv)]
                for i in range(nv):
                    ref[row, i * nv + k] = tree([block[i][j] * column[j] for j in range(nv)])
        return carry

    lax.fori_loop(0, rows, prepare, 0)

    def grow(row, carry):
        new = advance(low_steps, row, list(carry))
        for at in range(nn):
            grown[row, at] = new[at]
        return tuple(new)

    last = lax.fori_loop(0, rows, grow, tuple(identity))
    for at in range(nn):
        send_maps[pl.ds(at, cells, stride=EARLY), :] = last[at]

    def respond(index, carry):
        row = rows - 1 - index
        new = advance(up_steps, row, list(carry))
        return tuple(grown[row, at] + new[at] for at in range(nn))

    response = lax.fori_loop(0, rows, respond, tuple([zero] * nn))
    for at in range(nn):
        send_maps[pl.ds(nn + at, cells, stride=EARLY), :] = response[at]

    def shrink(index, carry):
        return tuple(advance(up_steps, rows - 1 - index, list(carry)))

    last = lax.fori_loop(0, rows, shrink, tuple(identity))
    for at in range(nn):
        send_maps[pl.ds(2 * nn + at, cells, stride=EARLY), :] = last[at]

    def to_owners(make):
        for k in range(owners):
            @pl.when(mine != first + k)
            def _(k=k):
                make(k).start()

    def late_copy(k):
        return remote(
            send_maps.at[pl.ds(late_row(k) * EARLY, MAPS), :], got_late.at[mine],
            late_send.at[k], late_recv.at[mine], {"span": first + k},
        )

    def early_copy(k):
        return remote(
            send_maps.at[pl.ds(early_row(k) * EARLY, EARLY), :], got_early.at[mine],
            early_send.at[k], early_recv.at[mine], {"span": first + k},
        )

    def pair_copy(k):
        return remote(
            send_pair.at[pl.ds(late_row(k) * PAIR, PAIR), :], got_pair.at[mine],
            pair_send.at[k], pair_recv.at[mine], {"span": first + k},
        )

    for copy in edge_copies:
        copy.wait_recv()
    from_left, from_right = edges[0], edges[1]
    for a in range(axial):
        for c in range(cw):
            groups = [[], [], [], []]
            for j in range(nv):
                at = j * axial + a
                here = tile(prior, j, a, c)
                if c > 0:
                    border = pltpu.roll(tile(prior, j, a, c - 1), 1, 1)
                else:
                    border = pltpu.roll(from_left, LANES - (nv * axial + at), 1)
                groups[0].append(jnp.where(lane == 0, border, pltpu.roll(here, 1, 1)))
                if c + 1 < cw:
                    border = pltpu.roll(tile(prior, j, a, c + 1), LANES - 1, 1)
                else:
                    border = pltpu.roll(from_right, LANES - 1 - at, 1)
                groups[1].append(
                    jnp.where(lane == LANES - 1, border, pltpu.roll(here, LANES - 1, 1)))
                if a > 0:
                    groups[2].append(tile(prior, j, a - 1, c))
                if a + 1 < axial:
                    groups[3].append(tile(prior, j, a + 1, c))
            for i in range(nv):
                value = tile(res, i, a, c)
                for side in range(4):
                    for j, neighbour in enumerate(groups[side]):
                        value = value - entry(2 + side, i, j) * neighbour
                at = ((i * axial + a) * cw + c) * rows
                src[at:at + rows, :] = value

    def forward(row, star):
        block = block_at(row)
        rhs = [cell_row(src, i, row) for i in range(nv)]
        known = times(block, rhs, nv)
        for i in range(nv):
            base[row, i] = known[i]
        moved = times(steps_at(low_steps, row), list(star), nv)
        star = [x + y for x, y in zip(known, moved)]
        for i in range(nv):
            grown[row, i] = star[i]
        return tuple(star)

    def backward(index, following):
        row = rows - 1 - index
        moved = times(steps_at(up_steps, row), list(following), nv)
        return tuple(grown[row, i] + moved[i] for i in range(nv))

    def local_sweeps():
        last = lax.fori_loop(0, rows, forward, tuple([zero] * nv))
        top = lax.fori_loop(0, rows, backward, tuple([zero] * nv))
        return list(last) + list(top)

    ends = local_sweeps()
    for at in range(2 * nv):
        send_maps[pl.ds(3 * nn + at, cells, stride=EARLY), :] = ends[at]
    to_owners(late_copy)
    to_owners(early_copy)

    get_char.wait()
    for at in range(2 * nn):
        entries[2 * at:2 * at + 2, :] = char[at]
    table = entries[...]
    part = harmonics // 4
    source_k = lax.broadcasted_iota(jnp.int32, (harmonics, harmonics), 0)
    target = lax.broadcasted_iota(jnp.int32, (harmonics, harmonics), 1)
    wanted = 4 * lax.rem(target, part) + target // part
    chosen = jnp.where(source_k == wanted, 1.0, 0.0).astype(BF16)
    picked = jnp.zeros(table.shape, F32)
    rest = table
    for _ in range(3):
        head = rest.astype(BF16)
        rest = rest - head.astype(F32)
        picked = picked + jnp.dot(head, chosen, preferred_element_type=F32)
    entries[...] = picked
    points = n * cw * LANES
    upper = lax.broadcasted_iota(jnp.int32, (2 * half, part), 0) >= half
    index = lax.broadcasted_iota(jnp.int32, (2 * half, part), 1)
    for s in range(4):
        k = 4 * index + s
        weight = jnp.where(k == 0, 1.0, 2.0).astype(F32) / points
        kept = jnp.where(upper, cutoffs[1], cutoffs[0])
        weight = jnp.where(k < kept, weight, 0.0)
        for i in range(nv):
            for j in range(nv):
                for p in range(2):
                    at0 = 2 * (i * nv + j) + p
                    at1 = at0 + 2 * nn
                    a = jnp.broadcast_to(entries[at0:at0 + 1, s * part:(s + 1) * part],
                                         (2 * half, part))
                    b = jnp.broadcast_to(entries[at1:at1 + 1, s * part:(s + 1) * part],
                                         (2 * half, part))
                    chars[s, 2 * (i * nv + j) + p] = jnp.where(upper, b, a) * weight

    get_fwd.wait()
    for copy in gather:
        copy.wait_recv()
    per_quarter = (points // 4) // LANES
    quarters = []
    for q in range(4):
        pieces = []
        for t in range(q * per_quarter, (q + 1) * per_quarter):
            d, c = t // cw, t % cw
            pieces.append(lines[d, c * count:(c + 1) * count, :])
        quarters.append(jnp.concatenate(pieces, axis=1))
    even0, even1 = quarters[0] + quarters[2], quarters[1] + quarters[3]
    odd0, odd1 = quarters[0] - quarters[2], quarters[1] - quarters[3]
    wide = 2 * part

    def onward(value, s):
        return split_dot(
            value, fwd[0, :, s * wide:(s + 1) * wide], fwd[1, :, s * wide:(s + 1) * wide])

    real, imag = [None] * 4, [None] * 4
    for s, value in ((0, even0 + even1), (2, even0 - even1)):
        both = onward(value, s)
        real[s], imag[s] = both[:, :part], -both[:, part:]
    odd = jnp.concatenate([odd0, odd1])
    both = onward(odd, 1)
    real[1] = both[:count, :part] - both[count:, part:]
    imag[1] = -(both[:count, part:] + both[count:, :part])
    both = onward(odd, 3)
    real[3] = both[:count, :part] + both[count:, part:]
    imag[3] = both[count:, :part] - both[:count, part:]

    new_real, new_imag = [], []
    group = 2 * half
    for s in range(4):
        sr = [real[s][j * group:(j + 1) * group] for j in range(nv)]
        si = [imag[s][j * group:(j + 1) * group] for j in range(nv)]
        outr, outi = [], []
        for i in range(nv):
            cr = [chars[s, 2 * (i * nv + j)] for j in range(nv)]
            ci = [chars[s, 2 * (i * nv + j) + 1] for j in range(nv)]
            outr.append(total([cr[j] * sr[j] - ci[j] * si[j] for j in range(nv)]))
            outi.append(total([cr[j] * si[j] + ci[j] * sr[j] for j in range(nv)]))
        new_real.append(jnp.concatenate(outr))
        new_imag.append(jnp.concatenate(outi))

    get_inv.wait()

    def homeward(value, s):
        return split_dot(
            value, inv[0, s * wide:(s + 1) * wide, :], inv[1, s * wide:(s + 1) * wide, :])

    def beside(a, b):
        return jnp.concatenate([a, b], axis=1)

    r0 = homeward(beside(new_real[0], -new_imag[0]), 0)
    r2 = homeward(beside(new_real[2], -new_imag[2]), 2)
    both1 = homeward(
        jnp.concatenate(
            [beside(new_real[1], -new_imag[1]), beside(-new_imag[1], -new_real[1])]), 1)
    both3 = homeward(
        jnp.concatenate(
            [beside(new_real[3], -new_imag[3]), beside(new_imag[3], new_real[3])]), 3)
    odd_real = both1[:count] + both3[:count]
    odd_imag = both1[count:] + both3[count:]
    spans = (2 * cw) // per_quarter
    if spans == 2:
        sign = (1 - 2 * chip).astype(F32)
        fields = [r0 + r2 + sign * odd_real, r0 - r2 + sign * odd_imag]
    else:
        sign = (1 - 2 * (chip // 2)).astype(F32)
        turned = lax.rem(chip, 2).astype(F32)
        straight = 1.0 - turned
        field = r0 + (straight - turned) * r2 + sign * (
            straight * odd_real + turned * odd_imag)
        fields = [field[:, c * cw * LANES:(c + 1) * cw * LANES] for c in range(2)]
    is_first = core == 0
    for c in range(cw):
        lo, hi = c * LANES, (c + 1) * LANES
        a, b = fields[0][:, lo:hi], fields[1][:, lo:hi]
        corr_send[c * count:(c + 1) * count, :] = jnp.where(is_first, b, a)
        corr_got[0, c * count:(c + 1) * count, :] = jnp.where(is_first, a, b)
    swap = remote(
        corr_send, corr_got.at[1], corr_ssem, corr_rsem, {"pitch": jnp.bitwise_xor(me, 1)})
    swap.start()
    swap.wait_recv()
    lower_rows = lax.broadcasted_iota(jnp.int32, (rows, LANES), 0) < half
    for c in range(cw):
        for i in range(nv):
            for q in range(2):
                a = 0 if q == 0 else axial - 1
                at = ((i * axial + a) * cw + c) * rows
                fr = c * count + i * group + q * half
                ours = corr_got[0, fr:fr + half, :]
                theirs = corr_got[1, fr:fr + half, :]
                src[at:at + half, :] += jnp.where(is_first, ours, theirs)
                src[at + half:at + rows, :] += jnp.where(is_first, theirs, ours)

    ends = local_sweeps()
    for at in range(2 * nv):
        send_pair[pl.ds(at, cells, stride=PAIR), :] = ends[at]
    to_owners(pair_copy)

    def solve(maps, terms, offset, solved):
        def mapped(d, start, vector):
            return tree(
                [maps[d, start + j * nv:start + (j + 1) * nv, :] * vector[j:j + 1]
                 for j in range(nv)])

        def term(d, which):
            return terms[d, offset + which * nv:offset + (which + 1) * nv, :]

        incoming = jnp.zeros((nv, LANES), F32)
        every = []
        for d in range(m):
            every.append(incoming)
            solved[d, 0:nv, :] = incoming
            if d + 1 < m:
                incoming = term(d, 0) + mapped(d, 0, incoming)
        following = jnp.zeros((nv, LANES), F32)
        for d in reversed(range(m)):
            solved[d, nv:2 * nv, :] = following
            if d > 0:
                known = term(d, 1) + mapped(d, nn, every[d])
                following = known + mapped(d, 2 * nn, following)

    def reply(solved, row, send, recv):
        out_copies = []
        for step in range(1, m):
            to = lax.rem(mine + step, m)
            out_copies.append(
                remote(
                    solved.at[to], back.at[pl.ds(pl.multiple_of(row * PAIR, 8), PAIR), :],
                    send.at[step - 1], recv.at[own], {"span": to}))
            out_copies[-1].start()
        back[pl.ds(pl.multiple_of(row * PAIR, 8), PAIR), :] = solved[mine]
        return out_copies

    def arrived(make_buffer, recv):
        for step in range(1, m):
            d = lax.rem(mine + step, m)
            remote(
                make_buffer.at[d], make_buffer.at[d], recv.at[d], recv.at[d], {"span": d}
            ).wait_recv()

    def own_rows(ref, row, stride, size):
        return ref[pl.ds(pl.multiple_of(row * stride, 8), size), :]

    @pl.when(is_owner)
    def _():
        late = late_row(own)
        early = early_row(own)
        got_early[mine] = own_rows(send_maps, early, EARLY, EARLY)
        got_late[mine] = own_rows(send_maps, late, EARLY, MAPS)
        got_pair[mine] = own_rows(send_pair, late, PAIR, PAIR)
        arrived(got_early, early_recv)
        solve(got_early, got_early, 3 * nn, solved_early)
        first_out = reply(solved_early, early, re_send, re_recv)
        arrived(got_late, late_recv)
        arrived(got_pair, pair_recv)
        solve(got_late, got_pair, 0, solved_late)
        second_out = reply(solved_late, late, rl_send, rl_recv)
        for copy in first_out + second_out:
            copy.wait_send()

    for k in range(owners):
        @pl.when(mine != first + k)
        def _(k=k):
            for row, recv in ((early_row(k), re_recv), (late_row(k), rl_recv)):
                place = back.at[pl.ds(row * PAIR, PAIR), :]
                remote(place, place, recv.at[k], recv.at[k], {"span": first + k}).wait_recv()

    incoming = [back[pl.ds(i, cells, stride=PAIR), :] for i in range(2 * nv)]

    def last_forward(row, star):
        moved = times(steps_at(low_steps, row), list(star), nv)
        star = [base[row, i] + moved[i] for i in range(nv)]
        for i in range(nv):
            grown[row, i] = star[i]
        return tuple(star)

    def last_backward(index, following):
        row = rows - 1 - index
        value = backward(index, following)
        for i in range(nv):
            out[pl.ds(i * cells * rows + row, cells, stride=rows), :] = value[i]
        return value

    lax.fori_loop(0, rows, last_forward, tuple(incoming[:nv]))
    lax.fori_loop(0, rows, last_backward, tuple(incoming[nv:]))

    for copy in gather + edge_copies + [swap]:
        copy.wait_send()
    for k in range(owners):
        @pl.when(mine != first + k)
        def _(k=k):
            for make in (late_copy, early_copy, pair_copy):
                make(k).wait_send()


def body(residual, inverse_diagonal, prior, coupling, characteristic, cutoffs):
    nv, axial, rows, width = residual.shape
    n = lax.axis_size("pitch")
    m = lax.axis_size("span")
    cw = width // LANES
    cells = axial * cw
    nn = nv * nv
    harmonics = characteristic.shape[2]
    points = n * width
    owners = 2 * cw
    half = rows // 2
    count = 2 * nv * half
    part = harmonics // 4

    def flat(field):
        field = field.reshape(field.shape[:-1] + (cw, LANES))
        return jnp.swapaxes(field, -2, -3).reshape(-1, LANES)

    fwd, inv = tables(points, harmonics)
    entries = characteristic.transpose(0, 3, 4, 1, 2).reshape(-1, 2, harmonics)
    smem = pl.BlockSpec(memory_space=SMEM)
    anywhere = pl.BlockSpec(memory_space=pl.ANY)
    field_rows = cells * rows
    update = pl.pallas_call(
        lambda *refs: kernel(nv, axial, rows, cw, harmonics, *refs),
        out_shape=VMEM((nv * field_rows, LANES), F32),
        in_specs=[smem, smem] + [anywhere] * 6,
        out_specs=pl.BlockSpec(memory_space=VMEM),
        scratch_shapes=[
            VMEM((nv * field_rows, LANES), F32),
            VMEM((nv * field_rows, LANES), F32),
            VMEM((nn * field_rows, LANES), F32),
            VMEM(entries.shape, F32),
            VMEM(fwd.shape, BF16),
            VMEM(inv.shape, BF16),
            VMEM((2, cw * count, LANES), F32),
            VMEM((n, cw * count, LANES), F32),
            VMEM((rows, LANES), F32),
            VMEM((2, rows, LANES), F32),
            VMEM((2 * entries.shape[0], harmonics), F32),
            VMEM((4, 2 * nn, 2 * half, part), F32),
            VMEM((rows, nn, cells, LANES), F32),
            VMEM((rows, nn, cells, LANES), F32),
            VMEM((rows, nn, cells, LANES), F32),
            VMEM((nv * field_rows, LANES), F32),
            VMEM((rows, nv, cells, LANES), F32),
            VMEM((cells * EARLY, LANES), F32),
            VMEM((cells * PAIR, LANES), F32),
            VMEM((m, MAPS, LANES), F32),
            VMEM((m, EARLY, LANES), F32),
            VMEM((m, PAIR, LANES), F32),
            VMEM((m, PAIR, LANES), F32),
            VMEM((m, PAIR, LANES), F32),
            VMEM((cells * PAIR, LANES), F32),
            VMEM((cw * count, LANES), F32),
            VMEM((2, cw * count, LANES), F32),
            DMA((6,)),
            DMA((n - 1,)),
            DMA((n - 1,)),
            DMA((2,)),
            DMA((2,)),
            DMA,
            DMA,
            DMA((owners,)),
            DMA((m,)),
            DMA((owners,)),
            DMA((m,)),
            DMA((owners,)),
            DMA((m,)),
            DMA((m - 1,)),
            DMA((owners,)),
            DMA((m - 1,)),
            DMA((owners,)),
        ],
        compiler_params=pltpu.CompilerParams(collective_id=0, has_side_effects=True),
        name="step",
    )(
        cutoffs,
        coupling.reshape(-1),
        flat(residual),
        flat(prior),
        flat(inverse_diagonal),
        entries,
        jnp.asarray(fwd),
        jnp.asarray(inv),
    )
    update = update.reshape(nv, axial, cw, rows, LANES)
    return jnp.swapaxes(update, 2, 3).reshape(nv, axial, rows, width)


def solution(mesh):
    in_specs = (
        P(None, None, "span", "pitch"),
        P(None, None, None, "span", "pitch"),
        P(None, None, "span", "pitch"),
        P(),
        P(),
        P(),
    )
    out_specs = P(None, None, "span", "pitch")
    return jax.shard_map(body, mesh=mesh, in_specs=in_specs, out_specs=out_specs, check_vma=False)
```

```python
import jax
import jax.numpy as jnp
import numpy as np
from jax import lax
from jax.experimental import pallas as pl
from jax.experimental.pallas import tpu as pltpu
from jax.sharding import PartitionSpec as P

LANES = 128
SUBLANES = 8
VMEM = pltpu.VMEM
SMEM = pltpu.SMEM
DMA = pltpu.SemaphoreType.DMA
MAPS = 80
PAIR = 16
F32 = jnp.float32
BF16 = jnp.bfloat16


def total(terms):
    result = terms[0]
    for term in terms[1:]:
        result = result + term
    return result


def tree(terms):
    while len(terms) > 1:
        terms = [
            terms[i] + terms[i + 1] if i + 1 < len(terms) else terms[i]
            for i in range(0, len(terms), 2)
        ]
    return terms[0]


def times(block, vector, nv):
    return [tree([block[i][j] * vector[j] for j in range(nv)]) for i in range(nv)]


def remote(src, dst, send, recv, device):
    return pltpu.make_async_remote_copy(
        src_ref=src,
        dst_ref=dst,
        send_sem=send,
        recv_sem=recv,
        device_id=device,
        device_id_type=pl.DeviceIdType.MESH,
    )


def split_dot(value, high, low):
    rows = value.shape[0]
    head = value.astype(BF16)
    rest = (value - head.astype(F32)).astype(BF16)
    both = jnp.dot(jnp.concatenate([head, rest]), high, preferred_element_type=F32)
    return both[:rows] + both[rows:] + jnp.dot(head, low, preferred_element_type=F32)


def tables(points, harmonics):
    quarter = points // 4
    p = np.arange(quarter)[:, None]
    blocks = []
    for s in range(4):
        angle = (p * (4 * np.arange(harmonics // 4)[None, :] + s) % points) * (2.0 * np.pi / points)
        blocks.append(np.concatenate([np.cos(angle), np.sin(angle)], axis=1))
    full = np.concatenate(blocks, axis=1).astype(np.float32)
    high = full.astype(BF16)
    low = (full - high.astype(np.float32)).astype(BF16)
    forward = np.stack([high, low])
    return forward, np.ascontiguousarray(forward.transpose(0, 2, 1))


def kernel(
    nv, axial, rows, cw, harmonics,
    cutoffs_in, coupling_in, res_in, prior_in, diag_in, char_in, fwd_in, inv_in,
    out,
    cutoffs, coupling, res, prior, diag, char, fwd, inv,
    stage, lines, edge, edges, entries, chars,
    low_steps, up_steps, grown, src, base, send_maps, send_first, send_pair,
    got_late, got_early, got_first, got_pair, solved_early, solved_late, back,
    corr_send, corr_got,
    in_sem, sent, replied, lines_got, edges_got, swap_got,
    late_got, early_got, first_got, pair_got, reply_got,
):
    n = lax.axis_size("pitch")
    m = lax.axis_size("span")
    me = lax.axis_index("pitch")
    mine = lax.axis_index("span")
    core = lax.rem(me, 2)
    chip = me // 2
    cells = axial * cw
    nn = nv * nv
    half = rows // 2
    count = nv * 2 * half
    owners = 2 * cw
    first = m // 2 - owners // 2
    own = mine - first
    is_owner = jnp.logical_and(own >= 0, own < owners)

    def late_row(k):
        return jnp.where(k < cw, k, cells - 2 * cw + k) if not isinstance(k, int) else (
            k if k < cw else cells - 2 * cw + k)

    def early_row(k):
        return cw + k

    copies = [
        pltpu.make_async_copy(a, b, in_sem.at[i])
        for i, (a, b) in enumerate(
            [(res_in, res), (prior_in, prior), (diag_in, diag), (coupling_in, coupling),
             (cutoffs_in, cutoffs), (char_in, char), (fwd_in, fwd), (inv_in, inv)]
        )
    ]
    for copy in copies:
        copy.start()
    get_res, get_prior, get_diag, get_coupling, get_cutoffs, get_char, get_fwd, get_inv = copies

    barrier = pltpu.get_barrier_semaphore()

    def greet(axis, to):
        pl.semaphore_signal(
            barrier, inc=1, device_id={axis: to}, device_id_type=pl.DeviceIdType.MESH
        )

    @pl.when(is_owner)
    def _():
        for step in range(1, m):
            greet("span", jnp.bitwise_xor(mine, step))

    @pl.when(jnp.logical_not(is_owner))
    def _():
        for k in range(owners):
            greet("span", first + k)

    for step in range(1, n):
        greet("pitch", jnp.bitwise_xor(me, step))

    def received(place, sem):
        remote(place, place, sem, sem, {"pitch": jnp.bitwise_xor(me, 1)}).wait_recv()

    def gone(place, sem):
        remote(place, place, sem, sem, {"pitch": jnp.bitwise_xor(me, 1)}).wait_send()

    def tile(ref, i, a, c):
        at = ((i * axial + a) * cw + c) * rows
        return ref[at:at + rows, :]

    get_res.wait()
    for h in range(2):
        for c in range(cw):
            for i in range(nv):
                for q in range(2):
                    a = 0 if q == 0 else axial - 1
                    at = ((i * axial + a) * cw + c) * rows + h * half
                    to = c * count + i * 2 * half + q * half
                    stage[h, to:to + half, :] = res[at:at + half, :]

    get_prior.wait()
    lane = lax.broadcasted_iota(jnp.int32, (rows, LANES), 1)
    packed = jnp.zeros((rows, LANES), F32)
    for j in range(nv):
        for a in range(axial):
            at = j * axial + a
            left = jnp.broadcast_to(tile(prior, j, a, 0)[:, 0:1], (rows, LANES))
            right = jnp.broadcast_to(tile(prior, j, a, cw - 1)[:, LANES - 1:], (rows, LANES))
            packed = jnp.where(lane == at, left, packed)
            packed = jnp.where(lane == nv * axial + at, right, packed)
    edge[...] = packed

    get_diag.wait()
    get_coupling.wait()
    zero = jnp.zeros((cells, LANES), F32)
    one = jnp.ones((cells, LANES), F32)
    identity = [one if i == j else zero for j in range(nv) for i in range(nv)]

    def cell_row(ref, at, row):
        return ref[pl.ds(at * cells * rows + row, cells, stride=rows), :]

    def block_at(row):
        return [[cell_row(diag, i * nv + j, row) for j in range(nv)] for i in range(nv)]

    def entry(which, i, j):
        return coupling[i, which, j]

    def steps_at(ref, row):
        return [[ref[row, i * nv + j] for j in range(nv)] for i in range(nv)]

    def advance(ref, row, carry):
        step = steps_at(ref, row)
        new = []
        for j in range(nv):
            new += times(step, carry[j * nv:(j + 1) * nv], nv)
        return new

    def prepare(row, carry):
        block = block_at(row)
        for ref, which in ((low_steps, 0), (up_steps, 1)):
            for k in range(nv):
                column = [-entry(which, j, k) for j in range(nv)]
                for i in range(nv):
                    ref[row, i * nv + k] = tree([block[i][j] * column[j] for j in range(nv)])
        return carry

    lax.fori_loop(0, rows, prepare, 0)

    def grow(row, carry):
        new = advance(low_steps, row, list(carry))
        for at in range(nn):
            grown[row, at] = new[at]
        return tuple(new)

    last = lax.fori_loop(0, rows, grow, tuple(identity))
    for at in range(nn):
        send_maps[pl.ds(at, cells, stride=MAPS), :] = last[at]

    @pl.when(is_owner)
    def _():
        pl.semaphore_wait(barrier, n - 1 + m - 1)

    @pl.when(jnp.logical_not(is_owner))
    def _():
        pl.semaphore_wait(barrier, n - 1 + owners)

    after = lax.rem(me + 1, n)
    before = lax.rem(me + n - 1, n)
    remote(edge, edges.at[0], sent, edges_got, {"pitch": after}).start()
    remote(edge, edges.at[1], sent, edges_got, {"pitch": before}).start()
    for step in [s for s in range(2, n)] + [1]:
        to = jnp.bitwise_xor(me, step)
        remote(stage.at[lax.rem(to, 2)], lines.at[me], sent, lines_got, {"pitch": to}).start()
    lines[me] = stage[core]


    def respond(index, carry):
        row = rows - 1 - index
        new = advance(up_steps, row, list(carry))
        return tuple(grown[row, at] + new[at] for at in range(nn))

    response = lax.fori_loop(0, rows, respond, tuple([zero] * nn))
    for at in range(nn):
        send_maps[pl.ds(nn + at, cells, stride=MAPS), :] = response[at]

    def shrink(index, carry):
        return tuple(advance(up_steps, rows - 1 - index, list(carry)))

    last = lax.fori_loop(0, rows, shrink, tuple(identity))
    for at in range(nn):
        send_maps[pl.ds(2 * nn + at, cells, stride=MAPS), :] = last[at]

    def to_owners(make):
        for k in range(owners):
            @pl.when(mine != first + k)
            def _(k=k):
                make(k).start()

    def maps_copy(got, row, sem):
        return lambda k: remote(
            send_maps.at[pl.ds(row(k) * MAPS, 3 * nn), :], got.at[mine, pl.ds(0, 3 * nn), :],
            sent, sem, {"span": first + k},
        )

    def ends_copy(send, got, row, sem):
        return lambda k: remote(
            send.at[pl.ds(row(k) * PAIR, 2 * nv), :], got.at[mine, pl.ds(0, 2 * nv), :],
            sent, sem, {"span": first + k},
        )

    to_owners(maps_copy(got_late, late_row, late_got))
    to_owners(maps_copy(got_early, early_row, early_got))

    get_char.wait()
    get_cutoffs.wait()
    for at in range(2 * nn):
        entries[2 * at:2 * at + 2, :] = char[at]
    table = entries[...]
    part = harmonics // 4
    source_k = lax.broadcasted_iota(jnp.int32, (harmonics, harmonics), 0)
    target = lax.broadcasted_iota(jnp.int32, (harmonics, harmonics), 1)
    wanted = 4 * lax.rem(target, part) + target // part
    chosen = jnp.where(source_k == wanted, 1.0, 0.0).astype(BF16)
    picked = jnp.zeros(table.shape, F32)
    rest = table
    for _ in range(3):
        head = rest.astype(BF16)
        rest = rest - head.astype(F32)
        picked = picked + jnp.dot(head, chosen, preferred_element_type=F32)
    entries[...] = picked
    points = n * cw * LANES
    upper = lax.broadcasted_iota(jnp.int32, (2 * half, part), 0) >= half
    index = lax.broadcasted_iota(jnp.int32, (2 * half, part), 1)
    for s in range(4):
        k = 4 * index + s
        weight = jnp.where(k == 0, 1.0, 2.0).astype(F32) / points
        kept = jnp.where(upper, cutoffs[1], cutoffs[0])
        weight = jnp.where(k < kept, weight, 0.0)
        for i in range(nv):
            for j in range(nv):
                for p in range(2):
                    at0 = 2 * (i * nv + j) + p
                    at1 = at0 + 2 * nn
                    a = jnp.broadcast_to(entries[at0:at0 + 1, s * part:(s + 1) * part],
                                         (2 * half, part))
                    b = jnp.broadcast_to(entries[at1:at1 + 1, s * part:(s + 1) * part],
                                         (2 * half, part))
                    chars[s, 2 * (i * nv + j) + p] = jnp.where(upper, b, a) * weight

    received(edges, edges_got)
    from_left, from_right = edges[0], edges[1]
    for a in range(axial):
        for c in range(cw):
            groups = [[], [], [], []]
            for j in range(nv):
                at = j * axial + a
                here = tile(prior, j, a, c)
                if c > 0:
                    border = pltpu.roll(tile(prior, j, a, c - 1), 1, 1)
                else:
                    border = pltpu.roll(from_left, LANES - (nv * axial + at), 1)
                groups[0].append(jnp.where(lane == 0, border, pltpu.roll(here, 1, 1)))
                if c + 1 < cw:
                    border = pltpu.roll(tile(prior, j, a, c + 1), LANES - 1, 1)
                else:
                    border = pltpu.roll(from_right, LANES - 1 - at, 1)
                groups[1].append(
                    jnp.where(lane == LANES - 1, border, pltpu.roll(here, LANES - 1, 1)))
                if a > 0:
                    groups[2].append(tile(prior, j, a - 1, c))
                if a + 1 < axial:
                    groups[3].append(tile(prior, j, a + 1, c))
            for i in range(nv):
                value = tile(res, i, a, c)
                for side in range(4):
                    for j, neighbour in enumerate(groups[side]):
                        value = value - entry(2 + side, i, j) * neighbour
                at = ((i * axial + a) * cw + c) * rows
                src[at:at + rows, :] = value

    def backward(following, row):
        moved = times(steps_at(up_steps, row), following, nv)
        return [grown[row, i] + moved[i] for i in range(nv)]

    def local_sweeps(send):
        star = None
        for row in range(rows):
            block = block_at(row)
            known = times(block, [cell_row(src, i, row) for i in range(nv)], nv)
            for i in range(nv):
                base[row, i] = known[i]
            if star is not None:
                moved = times(steps_at(low_steps, row), star, nv)
                known = [x + y for x, y in zip(known, moved)]
            star = known
            for i in range(nv):
                grown[row, i] = star[i]
        following = star
        for row in reversed(range(rows - 1)):
            following = backward(following, row)
        for at, value in enumerate(star + following):
            send[pl.ds(at, cells, stride=PAIR), :] = value

    local_sweeps(send_first)
    to_owners(ends_copy(send_first, got_first, early_row, first_got))

    get_fwd.wait()
    received(lines.at[pl.ds(0, n - 1)], lines_got)
    per_quarter = (points // 4) // LANES
    quarters = []
    for q in range(4):
        pieces = []
        for t in range(q * per_quarter, (q + 1) * per_quarter):
            d, c = t // cw, t % cw
            pieces.append(lines[d, c * count:(c + 1) * count, :])
        quarters.append(jnp.concatenate(pieces, axis=1))
    even0, even1 = quarters[0] + quarters[2], quarters[1] + quarters[3]
    odd0, odd1 = quarters[0] - quarters[2], quarters[1] - quarters[3]
    wide = 2 * part

    def onward(value, s):
        return split_dot(
            value, fwd[0, :, s * wide:(s + 1) * wide], fwd[1, :, s * wide:(s + 1) * wide])

    real, imag = [None] * 4, [None] * 4
    for s, value in ((0, even0 + even1), (2, even0 - even1)):
        both = onward(value, s)
        real[s], imag[s] = both[:, :part], -both[:, part:]
    odd = jnp.concatenate([odd0, odd1])
    both = onward(odd, 1)
    real[1] = both[:count, :part] - both[count:, part:]
    imag[1] = -(both[:count, part:] + both[count:, :part])
    both = onward(odd, 3)
    real[3] = both[:count, :part] + both[count:, part:]
    imag[3] = both[count:, :part] - both[:count, part:]

    new_real, new_imag = [], []
    group = 2 * half
    for s in range(4):
        sr = [real[s][j * group:(j + 1) * group] for j in range(nv)]
        si = [imag[s][j * group:(j + 1) * group] for j in range(nv)]
        outr, outi = [], []
        for i in range(nv):
            cr = [chars[s, 2 * (i * nv + j)] for j in range(nv)]
            ci = [chars[s, 2 * (i * nv + j) + 1] for j in range(nv)]
            outr.append(total([cr[j] * sr[j] - ci[j] * si[j] for j in range(nv)]))
            outi.append(total([cr[j] * si[j] + ci[j] * sr[j] for j in range(nv)]))
        new_real.append(jnp.concatenate(outr))
        new_imag.append(jnp.concatenate(outi))

    get_inv.wait()

    def homeward(value, s):
        return split_dot(
            value, inv[0, s * wide:(s + 1) * wide, :], inv[1, s * wide:(s + 1) * wide, :])

    def beside(a, b):
        return jnp.concatenate([a, b], axis=1)

    r0 = homeward(beside(new_real[0], -new_imag[0]), 0)
    r2 = homeward(beside(new_real[2], -new_imag[2]), 2)
    both1 = homeward(
        jnp.concatenate(
            [beside(new_real[1], -new_imag[1]), beside(-new_imag[1], -new_real[1])]), 1)
    both3 = homeward(
        jnp.concatenate(
            [beside(new_real[3], -new_imag[3]), beside(new_imag[3], new_real[3])]), 3)
    odd_real = both1[:count] + both3[:count]
    odd_imag = both1[count:] + both3[count:]
    spans = (2 * cw) // per_quarter
    if spans == 2:
        sign = (1 - 2 * chip).astype(F32)
        fields = [r0 + r2 + sign * odd_real, r0 - r2 + sign * odd_imag]
    else:
        sign = (1 - 2 * (chip // 2)).astype(F32)
        turned = lax.rem(chip, 2).astype(F32)
        straight = 1.0 - turned
        field = r0 + (straight - turned) * r2 + sign * (
            straight * odd_real + turned * odd_imag)
        fields = [field[:, c * cw * LANES:(c + 1) * cw * LANES] for c in range(2)]
    is_first = core == 0
    for c in range(cw):
        lo, hi = c * LANES, (c + 1) * LANES
        a, b = fields[0][:, lo:hi], fields[1][:, lo:hi]
        corr_send[c * count:(c + 1) * count, :] = jnp.where(is_first, b, a)
        corr_got[0, c * count:(c + 1) * count, :] = jnp.where(is_first, a, b)
    swap = remote(
        corr_send, corr_got.at[1], sent, swap_got, {"pitch": jnp.bitwise_xor(me, 1)})
    swap.start()
    swap.wait_recv()
    lower_rows = lax.broadcasted_iota(jnp.int32, (rows, LANES), 0) < half
    for c in range(cw):
        for i in range(nv):
            for q in range(2):
                a = 0 if q == 0 else axial - 1
                at = ((i * axial + a) * cw + c) * rows
                fr = c * count + i * group + q * half
                ours = corr_got[0, fr:fr + half, :]
                theirs = corr_got[1, fr:fr + half, :]
                src[at:at + half, :] += jnp.where(is_first, ours, theirs)
                src[at + half:at + rows, :] += jnp.where(is_first, theirs, ours)

    local_sweeps(send_pair)
    to_owners(ends_copy(send_pair, got_pair, late_row, pair_got))

    def solve(maps, terms, solved):
        def mapped(d, start, vector):
            return tree(
                [maps[d, start + j * nv:start + (j + 1) * nv, :] * vector[j:j + 1]
                 for j in range(nv)])

        def term(d, which):
            return terms[d, which * nv:(which + 1) * nv, :]

        incoming = jnp.zeros((nv, LANES), F32)
        every = []
        for d in range(m):
            every.append(incoming)
            solved[d, 0:nv, :] = incoming
            if d + 1 < m:
                incoming = term(d, 0) + mapped(d, 0, incoming)
        following = jnp.zeros((nv, LANES), F32)
        for d in reversed(range(m)):
            solved[d, nv:2 * nv, :] = following
            if d > 0:
                known = term(d, 1) + mapped(d, nn, every[d])
                following = known + mapped(d, 2 * nn, following)

    def reply(solved, row):
        place = back.at[pl.ds(pl.multiple_of(row * PAIR, 8), 2 * nv), :]
        for step in range(1, m):
            to = jnp.bitwise_xor(mine, step)
            remote(
                solved.at[to, pl.ds(0, 2 * nv), :], place, replied, reply_got, {"span": to}
            ).start()
        place[...] = solved[mine, 0:2 * nv, :]

    def own_rows(ref, row, stride, size):
        return ref[pl.ds(pl.multiple_of(row * stride, 8), size), :]

    @pl.when(is_owner)
    def _():
        late = late_row(own)
        early = early_row(own)
        got_early[mine] = own_rows(send_maps, early, MAPS, MAPS)
        got_late[mine] = own_rows(send_maps, late, MAPS, MAPS)
        got_first[mine] = own_rows(send_first, early, PAIR, PAIR)
        got_pair[mine] = own_rows(send_pair, late, PAIR, PAIR)
        received(got_early.at[pl.ds(0, m - 1), pl.ds(0, 3 * nn), :], early_got)
        received(got_first.at[pl.ds(0, m - 1), pl.ds(0, 2 * nv), :], first_got)
        solve(got_early, got_first, solved_early)
        reply(solved_early, early)
        received(got_late.at[pl.ds(0, m - 1), pl.ds(0, 3 * nn), :], late_got)
        received(got_pair.at[pl.ds(0, m - 1), pl.ds(0, 2 * nv), :], pair_got)
        solve(got_late, got_pair, solved_late)
        reply(solved_late, late)
        gone(diag.at[pl.ds(0, 2 * (m - 1) * 2 * nv), :], replied)
        received(diag.at[pl.ds(0, 2 * (owners - 1) * 2 * nv), :], reply_got)

    @pl.when(jnp.logical_not(is_owner))
    def _():
        received(diag.at[pl.ds(0, 2 * owners * 2 * nv), :], reply_got)

    incoming = [back[pl.ds(i, cells, stride=PAIR), :] for i in range(2 * nv)]
    star = incoming[:nv]
    for row in range(rows):
        moved = times(steps_at(low_steps, row), star, nv)
        star = [base[row, i] + moved[i] for i in range(nv)]
        for i in range(nv):
            grown[row, i] = star[i]
    following = incoming[nv:]
    for row in reversed(range(rows)):
        following = backward(following, row)
        for i in range(nv):
            out[pl.ds(i * cells * rows + row, cells, stride=rows), :] = following[i]

    common = (n - 1) * cw * count + 2 * rows + cw * count
    each = 2 * (3 * nn + 2 * nv)

    @pl.when(is_owner)
    def _():
        gone(diag.at[pl.ds(0, common + (owners - 1) * each), :], sent)

    @pl.when(jnp.logical_not(is_owner))
    def _():
        gone(diag.at[pl.ds(0, common + owners * each), :], sent)


def body(residual, inverse_diagonal, prior, coupling, characteristic, cutoffs):
    nv, axial, rows, width = residual.shape
    n = lax.axis_size("pitch")
    m = lax.axis_size("span")
    cw = width // LANES
    cells = axial * cw
    nn = nv * nv
    harmonics = characteristic.shape[2]
    points = n * width
    owners = 2 * cw
    half = rows // 2
    count = 2 * nv * half
    part = harmonics // 4

    def flat(field):
        field = field.reshape(field.shape[:-1] + (cw, LANES))
        return jnp.swapaxes(field, -2, -3).reshape(-1, LANES)

    fwd, inv = tables(points, harmonics)
    entries = characteristic.transpose(0, 3, 4, 1, 2).reshape(-1, 2, harmonics)
    anywhere = pl.BlockSpec(memory_space=pl.ANY)
    field_rows = cells * rows
    update = pl.pallas_call(
        lambda *refs: kernel(nv, axial, rows, cw, harmonics, *refs),
        out_shape=VMEM((nv * field_rows, LANES), F32),
        in_specs=[anywhere] * 8,
        out_specs=pl.BlockSpec(memory_space=VMEM),
        scratch_shapes=[
            SMEM((2,), jnp.int32),
            SMEM((nv, 6, nv), F32),
            VMEM((nv * field_rows, LANES), F32),
            VMEM((nv * field_rows, LANES), F32),
            VMEM((nn * field_rows, LANES), F32),
            VMEM(entries.shape, F32),
            VMEM(fwd.shape, BF16),
            VMEM(inv.shape, BF16),
            VMEM((2, cw * count, LANES), F32),
            VMEM((n, cw * count, LANES), F32),
            VMEM((rows, LANES), F32),
            VMEM((2, rows, LANES), F32),
            VMEM((2 * entries.shape[0], harmonics), F32),
            VMEM((4, 2 * nn, 2 * half, part), F32),
            VMEM((rows, nn, cells, LANES), F32),
            VMEM((rows, nn, cells, LANES), F32),
            VMEM((rows, nn, cells, LANES), F32),
            VMEM((nv * field_rows, LANES), F32),
            VMEM((rows, nv, cells, LANES), F32),
            VMEM((cells * MAPS, LANES), F32),
            VMEM((cells * PAIR, LANES), F32),
            VMEM((cells * PAIR, LANES), F32),
            VMEM((m, MAPS, LANES), F32),
            VMEM((m, MAPS, LANES), F32),
            VMEM((m, PAIR, LANES), F32),
            VMEM((m, PAIR, LANES), F32),
            VMEM((m, PAIR, LANES), F32),
            VMEM((m, PAIR, LANES), F32),
            VMEM((cells * PAIR, LANES), F32),
            VMEM((cw * count, LANES), F32),
            VMEM((2, cw * count, LANES), F32),
            DMA((8,)),
            DMA,
            DMA,
            DMA,
            DMA,
            DMA,
            DMA,
            DMA,
            DMA,
            DMA,
            DMA,
        ],
        compiler_params=pltpu.CompilerParams(collective_id=0, has_side_effects=True),
        name="step",
    )(
        cutoffs,
        coupling.transpose(1, 0, 2),
        flat(residual),
        flat(prior),
        flat(inverse_diagonal),
        entries,
        jnp.asarray(fwd),
        jnp.asarray(inv),
    )
    update = update.reshape(nv, axial, cw, rows, LANES)
    return jnp.swapaxes(update, 2, 3).reshape(nv, axial, rows, width)


def solution(mesh):
    in_specs = (
        P(None, None, "span", "pitch"),
        P(None, None, None, "span", "pitch"),
        P(None, None, "span", "pitch"),
        P(),
        P(),
        P(),
    )
    out_specs = P(None, None, "span", "pitch")
    return jax.shard_map(body, mesh=mesh, in_specs=in_specs, out_specs=out_specs, check_vma=False)
```

```python
import jax
import jax.numpy as jnp
import numpy as np
from jax import lax
from jax.experimental import pallas as pl
from jax.experimental.pallas import tpu as pltpu
from jax.sharding import PartitionSpec as P

LANES = 128
SUBLANES = 8
VMEM = pltpu.VMEM
SMEM = pltpu.SMEM
DMA = pltpu.SemaphoreType.DMA
MAPS = 80
PAIR = 16
F32 = jnp.float32
BF16 = jnp.bfloat16


def total(terms):
    result = terms[0]
    for term in terms[1:]:
        result = result + term
    return result


def tree(terms):
    while len(terms) > 1:
        terms = [
            terms[i] + terms[i + 1] if i + 1 < len(terms) else terms[i]
            for i in range(0, len(terms), 2)
        ]
    return terms[0]


def times(block, vector, nv):
    return [tree([block[i][j] * vector[j] for j in range(nv)]) for i in range(nv)]


def remote(src, dst, send, recv, device):
    return pltpu.make_async_remote_copy(
        src_ref=src,
        dst_ref=dst,
        send_sem=send,
        recv_sem=recv,
        device_id=device,
        device_id_type=pl.DeviceIdType.MESH,
    )


def split_dot(value, high, low):
    rows = value.shape[0]
    head = value.astype(BF16)
    rest = (value - head.astype(F32)).astype(BF16)
    both = jnp.dot(jnp.concatenate([head, rest]), high, preferred_element_type=F32)
    return both[:rows] + both[rows:] + jnp.dot(head, low, preferred_element_type=F32)


def tables(points, harmonics):
    quarter = points // 4
    p = np.arange(quarter)[:, None]
    blocks = []
    for s in range(4):
        angle = (p * (4 * np.arange(harmonics // 4)[None, :] + s) % points) * (2.0 * np.pi / points)
        blocks.append(np.concatenate([np.cos(angle), np.sin(angle)], axis=1))
    full = np.concatenate(blocks, axis=1).astype(np.float32)
    high = full.astype(BF16)
    low = (full - high.astype(np.float32)).astype(BF16)
    forward = np.stack([high, low])
    return forward, np.ascontiguousarray(forward.transpose(0, 2, 1))


def kernel(
    nv, axial, rows, cw, harmonics,
    cutoffs_in, coupling_in, res_in, prior_in, diag_in, char_in, fwd_in, inv_in,
    out,
    cutoffs, coupling, res, prior, diag, char, fwd, inv,
    stage, lines, edge, edges, entries, chars,
    low_steps, up_steps, grown, src, base, send_maps, send_first, send_pair,
    got_maps, got_first, got_pair, solved_early, solved_late, back,
    corr_send, corr_got,
    in_sem, sent, replied, lines_got, edges_got, swap_got,
    maps_got, first_got, pair_got, reply_got,
):
    n = lax.axis_size("pitch")
    m = lax.axis_size("span")
    me = lax.axis_index("pitch")
    mine = lax.axis_index("span")
    core = lax.rem(me, 2)
    chip = me // 2
    cells = axial * cw
    nn = nv * nv
    half = rows // 2
    count = nv * 2 * half
    owners = 2 * cw
    first = m // 2 - owners // 2
    own = mine - first
    is_owner = jnp.logical_and(own >= 0, own < owners)

    def late_row(k):
        return jnp.where(k < cw, k, cells - 2 * cw + k) if not isinstance(k, int) else (
            k if k < cw else cells - 2 * cw + k)

    def early_row(k):
        return cw + k

    copies = [
        pltpu.make_async_copy(a, b, in_sem.at[i])
        for i, (a, b) in enumerate(
            [(res_in, res), (prior_in, prior), (diag_in, diag), (coupling_in, coupling),
             (cutoffs_in, cutoffs), (char_in, char), (fwd_in, fwd), (inv_in, inv)]
        )
    ]
    for copy in copies:
        copy.start()
    get_res, get_prior, get_diag, get_coupling, get_cutoffs, get_char, get_fwd, get_inv = copies

    barrier = pltpu.get_barrier_semaphore()

    def greet(axis, to):
        pl.semaphore_signal(
            barrier, inc=1, device_id={axis: to}, device_id_type=pl.DeviceIdType.MESH
        )

    @pl.when(is_owner)
    def _():
        for step in range(1, m):
            greet("span", jnp.bitwise_xor(mine, step))

    @pl.when(jnp.logical_not(is_owner))
    def _():
        for k in range(owners):
            greet("span", first + k)

    for step in range(1, n):
        greet("pitch", jnp.bitwise_xor(me, step))

    def received(place, sem):
        remote(place, place, sem, sem, {"pitch": jnp.bitwise_xor(me, 1)}).wait_recv()

    def gone(place, sem):
        remote(place, place, sem, sem, {"pitch": jnp.bitwise_xor(me, 1)}).wait_send()

    def tile(ref, i, a, c):
        at = ((i * axial + a) * cw + c) * rows
        return ref[at:at + rows, :]

    get_res.wait()
    for h in range(2):
        for c in range(cw):
            for i in range(nv):
                for q in range(2):
                    a = 0 if q == 0 else axial - 1
                    at = ((i * axial + a) * cw + c) * rows + h * half
                    to = c * count + i * 2 * half + q * half
                    stage[h, to:to + half, :] = res[at:at + half, :]

    @pl.when(is_owner)
    def _():
        pl.semaphore_wait(barrier, n - 1 + m - 1)

    @pl.when(jnp.logical_not(is_owner))
    def _():
        pl.semaphore_wait(barrier, n - 1 + owners)

    for step in [s for s in range(2, n)] + [1]:
        to = jnp.bitwise_xor(me, step)
        remote(stage.at[lax.rem(to, 2)], lines.at[me], sent, lines_got, {"pitch": to}).start()
    lines[me] = stage[core]


    get_prior.wait()
    lane = lax.broadcasted_iota(jnp.int32, (rows, LANES), 1)
    packed = jnp.zeros((rows, LANES), F32)
    for j in range(nv):
        for a in range(axial):
            at = j * axial + a
            left = jnp.broadcast_to(tile(prior, j, a, 0)[:, 0:1], (rows, LANES))
            right = jnp.broadcast_to(tile(prior, j, a, cw - 1)[:, LANES - 1:], (rows, LANES))
            packed = jnp.where(lane == at, left, packed)
            packed = jnp.where(lane == nv * axial + at, right, packed)
    edge[...] = packed

    after = lax.rem(me + 1, n)
    before = lax.rem(me + n - 1, n)
    remote(edge, edges.at[0], sent, edges_got, {"pitch": after}).start()
    remote(edge, edges.at[1], sent, edges_got, {"pitch": before}).start()

    get_diag.wait()
    get_coupling.wait()

    def cell_row(ref, at, row):
        return ref[pl.ds(at * cells * rows + row, cells, stride=rows), :]

    def block_at(row):
        return [[cell_row(diag, i * nv + j, row) for j in range(nv)] for i in range(nv)]

    def entry(which, i, j):
        return coupling[i, which, j]

    def steps_at(ref, row):
        return [[ref[row, i * nv + j] for j in range(nv)] for i in range(nv)]

    def product(step, columns):
        result = []
        for j in range(nv):
            result += times(step, columns[j * nv:(j + 1) * nv], nv)
        return result

    def to_owners(make, sender=None):
        for k in range(owners):
            other = mine != first + k
            @pl.when(other if sender is None else jnp.logical_and(other, sender))
            def _(k=k):
                make(k).start()

    is_last = mine == m - 1
    is_inner = jnp.logical_and(mine > 0, mine < m - 1)

    def store_maps(start, values):
        for at, value in enumerate(values):
            send_maps[pl.ds(start + at, cells, stride=MAPS), :] = value

    def maps_copy(at, size):
        return lambda k: remote(
            send_maps.reshape(axial // 2, 2, cw, MAPS, LANES).at[
                k // cw, :, k % cw, pl.ds(at, size), :],
            got_maps.reshape(m, 2, MAPS, LANES).at[mine, :, pl.ds(at, size), :],
            sent, maps_got, {"span": first + k},
        )

    growth = None
    for row in range(rows):
        block = block_at(row)
        steps = []
        for ref, which in ((low_steps, 0), (up_steps, 1)):
            step = [[None] * nv for _ in range(nv)]
            for k in range(nv):
                column = [-entry(which, j, k) for j in range(nv)]
                for i in range(nv):
                    step[i][k] = tree([block[i][j] * column[j] for j in range(nv)])
                    ref[row, i * nv + k] = step[i][k]
            steps.append(step)
        if growth is None:
            growth = [steps[0][i][j] for j in range(nv) for i in range(nv)]
        else:
            growth = product(steps[0], growth)
        for at in range(nn):
            grown[row, at] = growth[at]
    store_maps(0, growth)
    to_owners(maps_copy(0, nn), is_inner)
    response = growth
    for row in reversed(range(rows - 1)):
        moved = product(steps_at(up_steps, row), response)
        response = [grown[row, at] + moved[at] for at in range(nn)]
    step = steps_at(up_steps, rows - 1)
    shrunk = [step[i][j] for j in range(nv) for i in range(nv)]
    for row in reversed(range(rows - 1)):
        shrunk = product(steps_at(up_steps, row), shrunk)
    store_maps(nn, response + shrunk)
    to_owners(maps_copy(nn, 2 * nn), is_inner)
    to_owners(maps_copy(nn, nn), is_last)

    def ends_copy(send, got, row, sem):
        return lambda k: remote(
            send.at[pl.ds(row(k) * PAIR, 2 * nv), :], got.at[mine, pl.ds(0, 2 * nv), :],
            sent, sem, {"span": first + k},
        )

    get_char.wait()
    get_cutoffs.wait()
    for at in range(2 * nn):
        entries[2 * at:2 * at + 2, :] = char[at]
    table = entries[...]
    part = harmonics // 4
    source_k = lax.broadcasted_iota(jnp.int32, (harmonics, harmonics), 0)
    target = lax.broadcasted_iota(jnp.int32, (harmonics, harmonics), 1)
    wanted = 4 * lax.rem(target, part) + target // part
    chosen = jnp.where(source_k == wanted, 1.0, 0.0).astype(BF16)
    picked = jnp.zeros(table.shape, F32)
    rest = table
    for _ in range(3):
        head = rest.astype(BF16)
        rest = rest - head.astype(F32)
        picked = picked + jnp.dot(head, chosen, preferred_element_type=F32)
    entries[...] = picked
    points = n * cw * LANES
    upper = lax.broadcasted_iota(jnp.int32, (2 * half, part), 0) >= half
    index = lax.broadcasted_iota(jnp.int32, (2 * half, part), 1)
    for s in range(4):
        k = 4 * index + s
        weight = jnp.where(k == 0, 1.0, 2.0).astype(F32) / points
        kept = jnp.where(upper, cutoffs[1], cutoffs[0])
        weight = jnp.where(k < kept, weight, 0.0)
        for i in range(nv):
            for j in range(nv):
                for p in range(2):
                    at0 = 2 * (i * nv + j) + p
                    at1 = at0 + 2 * nn
                    a = jnp.broadcast_to(entries[at0:at0 + 1, s * part:(s + 1) * part],
                                         (2 * half, part))
                    b = jnp.broadcast_to(entries[at1:at1 + 1, s * part:(s + 1) * part],
                                         (2 * half, part))
                    chars[s, 2 * (i * nv + j) + p] = jnp.where(upper, b, a) * weight

    get_fwd.wait()
    received(lines.at[pl.ds(0, n - 1)], lines_got)
    per_quarter = (points // 4) // LANES
    quarters = []
    for q in range(4):
        pieces = []
        for t in range(q * per_quarter, (q + 1) * per_quarter):
            d, c = t // cw, t % cw
            pieces.append(lines[d, c * count:(c + 1) * count, :])
        quarters.append(jnp.concatenate(pieces, axis=1))
    even0, even1 = quarters[0] + quarters[2], quarters[1] + quarters[3]
    odd0, odd1 = quarters[0] - quarters[2], quarters[1] - quarters[3]
    wide = 2 * part

    def onward(value, s):
        return split_dot(
            value, fwd[0, :, s * wide:(s + 1) * wide], fwd[1, :, s * wide:(s + 1) * wide])

    real, imag = [None] * 4, [None] * 4
    for s, value in ((0, even0 + even1), (2, even0 - even1)):
        both = onward(value, s)
        real[s], imag[s] = both[:, :part], -both[:, part:]
    odd = jnp.concatenate([odd0, odd1])
    both = onward(odd, 1)
    real[1] = both[:count, :part] - both[count:, part:]
    imag[1] = -(both[:count, part:] + both[count:, :part])
    both = onward(odd, 3)
    real[3] = both[:count, :part] + both[count:, part:]
    imag[3] = both[count:, :part] - both[:count, part:]

    new_real, new_imag = [], []
    group = 2 * half
    for s in range(4):
        sr = [real[s][j * group:(j + 1) * group] for j in range(nv)]
        si = [imag[s][j * group:(j + 1) * group] for j in range(nv)]
        outr, outi = [], []
        for i in range(nv):
            cr = [chars[s, 2 * (i * nv + j)] for j in range(nv)]
            ci = [chars[s, 2 * (i * nv + j) + 1] for j in range(nv)]
            outr.append(total([cr[j] * sr[j] - ci[j] * si[j] for j in range(nv)]))
            outi.append(total([cr[j] * si[j] + ci[j] * sr[j] for j in range(nv)]))
        new_real.append(jnp.concatenate(outr))
        new_imag.append(jnp.concatenate(outi))

    get_inv.wait()

    def homeward(value, s):
        return split_dot(
            value, inv[0, s * wide:(s + 1) * wide, :], inv[1, s * wide:(s + 1) * wide, :])

    def beside(a, b):
        return jnp.concatenate([a, b], axis=1)

    r0 = homeward(beside(new_real[0], -new_imag[0]), 0)
    r2 = homeward(beside(new_real[2], -new_imag[2]), 2)
    both1 = homeward(
        jnp.concatenate(
            [beside(new_real[1], -new_imag[1]), beside(-new_imag[1], -new_real[1])]), 1)
    both3 = homeward(
        jnp.concatenate(
            [beside(new_real[3], -new_imag[3]), beside(new_imag[3], new_real[3])]), 3)
    odd_real = both1[:count] + both3[:count]
    odd_imag = both1[count:] + both3[count:]
    spans = (2 * cw) // per_quarter
    if spans == 2:
        sign = (1 - 2 * chip).astype(F32)
        fields = [r0 + r2 + sign * odd_real, r0 - r2 + sign * odd_imag]
    else:
        sign = (1 - 2 * (chip // 2)).astype(F32)
        turned = lax.rem(chip, 2).astype(F32)
        straight = 1.0 - turned
        field = r0 + (straight - turned) * r2 + sign * (
            straight * odd_real + turned * odd_imag)
        fields = [field[:, c * cw * LANES:(c + 1) * cw * LANES] for c in range(2)]
    is_first = core == 0
    for c in range(cw):
        lo, hi = c * LANES, (c + 1) * LANES
        a, b = fields[0][:, lo:hi], fields[1][:, lo:hi]
        corr_send[c * count:(c + 1) * count, :] = jnp.where(is_first, b, a)
        corr_got[0, c * count:(c + 1) * count, :] = jnp.where(is_first, a, b)
    swap = remote(
        corr_send, corr_got.at[1], sent, swap_got, {"pitch": jnp.bitwise_xor(me, 1)})
    swap.start()

    received(edges, edges_got)
    from_left, from_right = edges[0], edges[1]
    for a in range(axial):
        for c in range(cw):
            groups = [[], [], [], []]
            for j in range(nv):
                at = j * axial + a
                here = tile(prior, j, a, c)
                if c > 0:
                    border = pltpu.roll(tile(prior, j, a, c - 1), 1, 1)
                else:
                    border = pltpu.roll(from_left, LANES - (nv * axial + at), 1)
                groups[0].append(jnp.where(lane == 0, border, pltpu.roll(here, 1, 1)))
                if c + 1 < cw:
                    border = pltpu.roll(tile(prior, j, a, c + 1), LANES - 1, 1)
                else:
                    border = pltpu.roll(from_right, LANES - 1 - at, 1)
                groups[1].append(
                    jnp.where(lane == LANES - 1, border, pltpu.roll(here, LANES - 1, 1)))
                if a > 0:
                    groups[2].append(tile(prior, j, a - 1, c))
                if a + 1 < axial:
                    groups[3].append(tile(prior, j, a + 1, c))
            for i in range(nv):
                value = tile(res, i, a, c)
                for side in range(4):
                    for j, neighbour in enumerate(groups[side]):
                        value = value - entry(2 + side, i, j) * neighbour
                at = ((i * axial + a) * cw + c) * rows
                src[at:at + rows, :] = value

    def backward(following, row):
        moved = times(steps_at(up_steps, row), following, nv)
        return [grown[row, i] + moved[i] for i in range(nv)]

    def local_sweeps(send):
        star = None
        for row in range(rows):
            block = block_at(row)
            known = times(block, [cell_row(src, i, row) for i in range(nv)], nv)
            for i in range(nv):
                base[row, i] = known[i]
            if star is not None:
                moved = times(steps_at(low_steps, row), star, nv)
                known = [x + y for x, y in zip(known, moved)]
            star = known
            for i in range(nv):
                grown[row, i] = star[i]
        following = star
        for row in reversed(range(rows - 1)):
            following = backward(following, row)
        for at, value in enumerate(star + following):
            send[pl.ds(at, cells, stride=PAIR), :] = value

    local_sweeps(send_first)
    to_owners(ends_copy(send_first, got_first, early_row, first_got))

    swap.wait_recv()
    lower_rows = lax.broadcasted_iota(jnp.int32, (rows, LANES), 0) < half
    for c in range(cw):
        for i in range(nv):
            for q in range(2):
                a = 0 if q == 0 else axial - 1
                at = ((i * axial + a) * cw + c) * rows
                fr = c * count + i * group + q * half
                ours = corr_got[0, fr:fr + half, :]
                theirs = corr_got[1, fr:fr + half, :]
                src[at:at + half, :] += jnp.where(is_first, ours, theirs)
                src[at + half:at + rows, :] += jnp.where(is_first, theirs, ours)

    local_sweeps(send_pair)
    to_owners(ends_copy(send_pair, got_pair, late_row, pair_got))

    def solve(slot, terms, solved):
        def mapped(d, start, vector):
            at = pl.multiple_of((2 * d + slot) * MAPS, 8) + start
            return tree(
                [got_maps[pl.ds(at + j * nv, nv), :] * vector[j:j + 1] for j in range(nv)])

        def term(d, which):
            return terms[d, which * nv:(which + 1) * nv, :]

        none = jnp.zeros((nv, LANES), F32)
        every = [none, term(0, 0)]
        for d in range(1, m - 1):
            every.append(term(d, 0) + mapped(d, 0, every[d]))
        following = none
        for d in reversed(range(m)):
            solved[d, 0:nv, :] = every[d]
            solved[d, nv:2 * nv, :] = following
            if d == m - 1:
                following = term(d, 1) + mapped(d, nn, every[d])
            elif d > 0:
                known = term(d, 1) + mapped(d, nn, every[d])
                following = known + mapped(d, 2 * nn, following)

    def reply(solved, row):
        place = back.at[pl.ds(pl.multiple_of(row * PAIR, 8), 2 * nv), :]
        for step in range(1, m):
            to = jnp.bitwise_xor(mine, step)
            remote(
                solved.at[to, pl.ds(0, 2 * nv), :], place, replied, reply_got, {"span": to}
            ).start()
        place[...] = solved[mine, 0:2 * nv, :]

    def own_rows(ref, row, stride, size):
        return ref[pl.ds(pl.multiple_of(row * stride, 8), size), :]

    @pl.when(is_owner)
    def _():
        late = late_row(own)
        early = early_row(own)
        side = own // cw
        for slot in range(2):
            row = (2 * side + slot) * cw + lax.rem(own, cw)
            place = pl.ds(pl.multiple_of((2 * mine + slot) * MAPS, 8), MAPS)
            got_maps[place, :] = own_rows(send_maps, row, MAPS, MAPS)
        got_first[mine] = own_rows(send_first, early, PAIR, PAIR)
        got_pair[mine] = own_rows(send_pair, late, PAIR, PAIR)
        received(got_maps.at[pl.ds(0, 2 * ((m - 3) * 3 * nn + nn)), :], maps_got)
        received(got_first.at[pl.ds(0, m - 1), pl.ds(0, 2 * nv), :], first_got)
        solve(1 - side, got_first, solved_early)
        reply(solved_early, early)
        received(got_pair.at[pl.ds(0, m - 1), pl.ds(0, 2 * nv), :], pair_got)
        solve(side, got_pair, solved_late)
        reply(solved_late, late)
        gone(diag.at[pl.ds(0, 2 * (m - 1) * 2 * nv), :], replied)
        received(diag.at[pl.ds(0, 2 * (owners - 1) * 2 * nv), :], reply_got)

    @pl.when(jnp.logical_not(is_owner))
    def _():
        received(diag.at[pl.ds(0, 2 * owners * 2 * nv), :], reply_got)

    incoming = [back[pl.ds(i, cells, stride=PAIR), :] for i in range(2 * nv)]
    star = incoming[:nv]
    for row in range(rows):
        moved = times(steps_at(low_steps, row), star, nv)
        star = [base[row, i] + moved[i] for i in range(nv)]
        for i in range(nv):
            grown[row, i] = star[i]
    following = incoming[nv:]
    for row in reversed(range(rows)):
        following = backward(following, row)
        for i in range(nv):
            out[pl.ds(i * cells * rows + row, cells, stride=rows), :] = following[i]

    common = (n - 1) * cw * count + 2 * rows + cw * count
    each = 2 * (3 * nn + 2 * nv)

    @pl.when(is_owner)
    def _():
        gone(diag.at[pl.ds(0, common + (owners - 1) * each), :], sent)

    for sender, size in (
        (jnp.logical_and(is_inner, jnp.logical_not(is_owner)), each),
        (mine == 0, each - 2 * 3 * nn),
        (is_last, each - 2 * (3 * nn - nn)),
    ):
        @pl.when(sender)
        def _(size=size):
            gone(diag.at[pl.ds(0, common + owners * size), :], sent)


def body(residual, inverse_diagonal, prior, coupling, characteristic, cutoffs):
    nv, axial, rows, width = residual.shape
    n = lax.axis_size("pitch")
    m = lax.axis_size("span")
    cw = width // LANES
    cells = axial * cw
    nn = nv * nv
    harmonics = characteristic.shape[2]
    points = n * width
    owners = 2 * cw
    half = rows // 2
    count = 2 * nv * half
    part = harmonics // 4

    def flat(field):
        field = field.reshape(field.shape[:-1] + (cw, LANES))
        return jnp.swapaxes(field, -2, -3).reshape(-1, LANES)

    fwd, inv = tables(points, harmonics)
    entries = characteristic.transpose(0, 3, 4, 1, 2).reshape(-1, 2, harmonics)
    anywhere = pl.BlockSpec(memory_space=pl.ANY)
    field_rows = cells * rows
    update = pl.pallas_call(
        lambda *refs: kernel(nv, axial, rows, cw, harmonics, *refs),
        out_shape=VMEM((nv * field_rows, LANES), F32),
        in_specs=[anywhere] * 8,
        out_specs=pl.BlockSpec(memory_space=VMEM),
        scratch_shapes=[
            SMEM((2,), jnp.int32),
            SMEM((nv, 6, nv), F32),
            VMEM((nv * field_rows, LANES), F32),
            VMEM((nv * field_rows, LANES), F32),
            VMEM((nn * field_rows, LANES), F32),
            VMEM(entries.shape, F32),
            VMEM(fwd.shape, BF16),
            VMEM(inv.shape, BF16),
            VMEM((2, cw * count, LANES), F32),
            VMEM((n, cw * count, LANES), F32),
            VMEM((rows, LANES), F32),
            VMEM((2, rows, LANES), F32),
            VMEM((2 * entries.shape[0], harmonics), F32),
            VMEM((4, 2 * nn, 2 * half, part), F32),
            VMEM((rows, nn, cells, LANES), F32),
            VMEM((rows, nn, cells, LANES), F32),
            VMEM((rows, nn, cells, LANES), F32),
            VMEM((nv * field_rows, LANES), F32),
            VMEM((rows, nv, cells, LANES), F32),
            VMEM((cells * MAPS, LANES), F32),
            VMEM((cells * PAIR, LANES), F32),
            VMEM((cells * PAIR, LANES), F32),
            VMEM((2 * m * MAPS, LANES), F32),
            VMEM((m, PAIR, LANES), F32),
            VMEM((m, PAIR, LANES), F32),
            VMEM((m, PAIR, LANES), F32),
            VMEM((m, PAIR, LANES), F32),
            VMEM((cells * PAIR, LANES), F32),
            VMEM((cw * count, LANES), F32),
            VMEM((2, cw * count, LANES), F32),
            DMA((8,)),
            DMA,
            DMA,
            DMA,
            DMA,
            DMA,
            DMA,
            DMA,
            DMA,
            DMA,
        ],
        compiler_params=pltpu.CompilerParams(collective_id=0, has_side_effects=True),
        name="step",
    )(
        cutoffs,
        coupling.transpose(1, 0, 2),
        flat(residual),
        flat(prior),
        flat(inverse_diagonal),
        entries,
        jnp.asarray(fwd),
        jnp.asarray(inv),
    )
    update = update.reshape(nv, axial, cw, rows, LANES)
    return jnp.swapaxes(update, 2, 3).reshape(nv, axial, rows, width)


def solution(mesh):
    in_specs = (
        P(None, None, "span", "pitch"),
        P(None, None, None, "span", "pitch"),
        P(None, None, "span", "pitch"),
        P(),
        P(),
        P(),
    )
    out_specs = P(None, None, "span", "pitch")
    return jax.shard_map(body, mesh=mesh, in_specs=in_specs, out_specs=out_specs, check_vma=False)
```
